32 devices in a mesh: row: 8 (over y, x, core), col: 4 (over z).
Axes of the slice: x: 2, y: 2, z: 4, core: 2. Of those that a mesh axis runs over, the one named last changes fastest.
Arguments:
- coeffs: bfloat16 [6144, 4096], P('row', 'col'), may hold values from -0.00390625 to 0.00390625
- occupation: float32 [4096], P('col'), may hold values from 0.5 to 2
- basis_on_grid: bfloat16 [320, 512, 512], P('row'), may hold values from -6 to 6
- basis_map: int32 [320, 512], P('row'), may hold values from 0 to 6143, as said below
- basis_count: int32 [320], P('row'), may hold values from 256 to 512
- batch_atom: int32 [320], P('row'), may hold values from 0 to 63
- harmonics: float32 [320, 49, 512], P('row'), may hold values from -0.25 to 0.25
Outputs:
- density: float32 [320, 512], P('row', 'col')
- moments: float32 [64, 49], replicated
The draws below stay inside these ranges and needn't reach their ends.
Inputs may be any that keep to these rules, and one draw needn't show every extreme that they name: `basis_map`: the slots of one batch name distinct basis functions. With R = 768 and o = b // 40, batch b names only basis functions q * R + (o * 96 + w) mod R with 0 <= q < 8 and 0 <= w < 96.
All inputs are finite; a program needn't handle non-finite values.
Results may differ from the reference program's by a relative error of at most 0.0003.
Values may be sent and summed in bfloat16 or wider, within the bound.
A program may use at most 192 MiB of HBM per device.

```python
import jax
import jax.numpy as jnp
from jax import lax

NB = 6144
NOCC = 4096
SLOTS = 512
WIN = 96
POINTS = 512
LM = 49
NATOM = 64
BD = 40
BATCHES = 320


def draw_basis_map(key, part):
    owners = BATCHES // BD
    shard = NB // owners
    keys = jax.random.split(jax.random.fold_in(key, 7), BATCHES)
    chosen = jax.vmap(lambda one: jax.random.permutation(one, WIN * owners))(keys)[:, :SLOTS]
    chosen = chosen.astype(jnp.int32)
    source = chosen // WIN
    offset = chosen % WIN
    owner = jnp.arange(BATCHES, dtype=jnp.int32) // BD
    local = jnp.mod(owner[:, None] * WIN + offset, shard)
    return (source * shard + local).astype(jnp.int32)


def set_ends(values, own_key, low, high):
    longest = values.shape.index(max(values.shape))
    spots = []
    for shift in (0, 1):
        where = [jax.random.randint(jax.random.fold_in(own_key, axis), (), 0, length) for axis, length in enumerate(values.shape)]
        where[longest] = (where[longest] + shift) % values.shape[longest]
        spots.append(tuple(where))
    return values.at[spots[0]].set(low).at[spots[1]].set(high)


def block_scale(own_key, extent, cuts, smallest, largest):
    gain, own = 1.0, jax.random.fold_in(own_key, 6)
    for position, shards_of in cuts:
        heights = jnp.exp(jax.random.uniform(jax.random.fold_in(own, position), (shards_of,), jnp.float32, smallest / len(cuts), largest / len(cuts)))
        gain = gain * jnp.repeat(heights, extent[position] // shards_of).reshape([-1 if axis == position else 1 for axis in range(len(extent))])
    return gain


def centred(rng, extent, deviation, limit, pieces=(), held_as=jnp.bfloat16):
    factor_of = block_scale(rng, extent, pieces, -0.22, 0.18) if pieces else 1.0
    entries = jax.random.normal(rng, extent, jnp.float32) * deviation * factor_of
    return jnp.minimum(jnp.maximum(entries, -limit), limit).astype(held_as)


def setup_inputs(seed: int = 0) -> dict:
    seeds = jax.random.split(jax.random.key(seed), 8)
    return {
        "coeffs": centred(seeds[0], (NB, NOCC), (SLOTS * NOCC) ** -0.5, 0.00390625, ((0, 8), (1, 4))),
        "occupation": jnp.clip(0.5 + 1.5 * jax.random.uniform(seeds[1], (NOCC,), jnp.float32) ** block_scale(seeds[1], (NOCC,), ((0, 4),), -0.2, 0.2), 0.5, 2.0),
        "basis_on_grid": centred(seeds[2], (BATCHES, POINTS, SLOTS), 1.0, 6.0, ((0, 8),)),
        "basis_map": draw_basis_map(jax.random.fold_in(seeds[7], 71), 0),
        "basis_count": set_ends(jax.random.randint(seeds[4], (BATCHES,), SLOTS // 2, SLOTS + 1), jax.random.fold_in(seeds[4], 1), SLOTS // 2, SLOTS).astype(jnp.int32),
        "batch_atom": set_ends(jax.random.randint(seeds[5], (BATCHES,), 0, NATOM), jax.random.fold_in(seeds[5], 1), 0, NATOM - 1).astype(jnp.int32),
        "harmonics": centred(seeds[6], (BATCHES, LM, POINTS), POINTS ** -0.5, 0.25, ((0, 8),), jnp.float32),
    }


def reference(coeffs, occupation, basis_on_grid, basis_map, basis_count, batch_atom, harmonics):
    slot_ids = jnp.arange(SLOTS, dtype=jnp.int32)

    def one_batch(items):
        values, indices, count = items
        selected = jnp.take(coeffs, indices, axis=0)
        keep = slot_ids < count
        masked = jnp.where(keep[None, :], values, jnp.zeros_like(values))
        orbital = jnp.dot(masked, selected, preferred_element_type=jnp.float32)
        return jnp.sum(occupation[None, :] * orbital * orbital, axis=1)

    density = lax.map(one_batch, (basis_on_grid, basis_map, basis_count))
    local_moment = jnp.einsum("blp,bp->bl", harmonics, density, precision=lax.Precision.HIGHEST)
    member = (batch_atom[:, None] == jnp.arange(NATOM, dtype=jnp.int32)[None, :]).astype(jnp.float32)
    moments = jnp.dot(member.T, local_moment, precision=lax.Precision.HIGHEST)
    return density, moments
```

```python
import functools

import jax
import jax.numpy as jnp
from jax import lax
from jax.experimental import pallas as pl
from jax.experimental.pallas import tpu as pltpu
from jax.sharding import PartitionSpec as P

WIN = 96
NATOM = 64
LANES = 128
VMEM_BYTES = 62 * 1024 * 1024
DEPTH = 4
STEPS = 32767.0
MARGIN = 1.0 + 2.0 ** -7
MESH = pl.DeviceIdType.MESH
ORDER = (0, 1, 2, 4, 3, 5, 6, 7)


def plain(coeffs, occupation, basis_on_grid, basis_map, basis_count):
    batches, points, slots = basis_on_grid.shape
    owned = coeffs.shape[0]
    owners = lax.axis_size("row")
    target = lax.broadcasted_iota(jnp.int32, (owners, WIN), 0)
    offset = lax.broadcasted_iota(jnp.int32, (owners, WIN), 1)
    outgoing_ids = jnp.mod(target * WIN + offset, owned).reshape(-1)
    outgoing = jnp.take(coeffs, outgoing_ids, axis=0)
    window = lax.all_to_all(outgoing, "row", split_axis=0, concat_axis=0, tiled=True)
    start = jnp.mod(lax.axis_index("row") * WIN, owned)
    source = basis_map // owned
    within = jnp.mod(basis_map % owned - start, owned)
    local_ids = source * WIN + within
    selected = jnp.take(window, local_ids, axis=0)
    slot_ids = lax.broadcasted_iota(jnp.int32, (batches, slots), 1)
    keep = slot_ids < basis_count[:, None]
    masked = jnp.where(keep[:, None, :], basis_on_grid, jnp.zeros_like(basis_on_grid))
    orbital = jnp.einsum("bps,bsk->bpk", masked, selected, preferred_element_type=jnp.float32)
    partial_density = jnp.sum(orbital * orbital * occupation[None, None, :], axis=2)
    full_density = lax.psum(partial_density, "col")
    share = points // lax.axis_size("col")
    return lax.dynamic_slice_in_dim(full_density, lax.axis_index("col") * share, share, 1)


def plan(groups, cols):
    early, late = groups - 1, groups - 1
    pairs = [[(i, (i, (i + 1) % early)) for i in range(early)]][0]
    rest = [(i, j) for i in range(early) for j in range(i) if (i - j) % early not in (1, early - 1)]
    while rest:
        degree = [sum(v in edge for edge in rest) for v in range(early)]
        v = degree.index(max(degree))
        taken = [edge for edge in rest if v in edge][:2]
        rest = [edge for edge in rest if edge not in taken]
        pairs.append((v, tuple(a if b == v else b for a, b in taken)))
    pairs.sort(key=lambda entry: -len(entry[1]))
    kept = [pairs[c::cols] for c in range(cols)]
    blocks = list(range(groups))
    counts = [groups // cols + (1 if c in range(0, 2 * (groups % cols), 2) else 0) for c in range(cols)]
    for c in range(cols):
        kept[c] = kept[c] + [(late, tuple(blocks[:counts[c]]))]
        blocks = blocks[counts[c]:]
    return kept


def kernel(rows, cols, owned, coeffs, occ, basis, index, count, atom, harmonics, out, out_moments,
           held, window, split, local, scale_col, scale_row, norm, code, taken, norms, matrix,
           spread, angular, member, line, dens, got, near, far, moment,
           own_sem, in_sem, angular_sem, send_sem, recv_sem, zsend_sem, zrecv_sem, vsend_sem, vrecv_sem,
           dsend_sem, drecv_sem, nsend_sem, nrecv_sem, fsend_sem, frecv_sem):
    batches, points, slots = basis.shape
    states = coeffs.shape[1]
    reach = rows * WIN
    groups = reach // LANES
    me, mine = lax.axis_index("row"), lax.axis_index("col")
    share = points // cols
    kept = plan(groups, cols)
    entries = len(kept[0])

    barrier = pltpu.get_barrier_semaphore()
    for k in range(1, rows):
        pl.semaphore_signal(barrier, inc=1, device_id={"row": lax.rem(me + k, rows)},
                            device_id_type=MESH)
    for k in range(1, cols):
        pl.semaphore_signal(barrier, inc=1, device_id={"col": lax.rem(mine + k, cols)},
                            device_id_type=MESH)

    def fetch(b, slot):
        return pltpu.make_async_copy(basis.at[b], held.at[slot], in_sem.at[slot])

    for b in range(DEPTH - 1):
        fetch(b, b).start()

    def rows_for(owner):
        return coeffs.at[pl.ds(pl.multiple_of(lax.rem(owner * WIN, owned), 32), WIN), :]

    def partner(k):
        bits = (lax.rem(me, 2), lax.rem(lax.div(me, 2), 2), lax.div(me, 4))
        return sum((1 - bit if k >> n & 1 else bit) * (1 << n) for n, bit in enumerate(bits))

    own = pltpu.make_async_copy(rows_for(me), window.at[0:WIN, :], own_sem)
    own.start()
    pl.semaphore_wait(barrier, rows + cols - 2)
    sends = []
    for p in range(1, rows):
        peer = partner(ORDER[p])
        copy = pltpu.make_async_remote_copy(
            src_ref=rows_for(peer), dst_ref=window.at[p * WIN:(p + 1) * WIN, :],
            send_sem=send_sem.at[p - 1], recv_sem=recv_sem.at[p - 1],
            device_id={"row": peer}, device_id_type=MESH)
        copy.start()
        sends.append(copy)
    load = pltpu.make_async_copy(harmonics, angular, angular_sem)
    load.start()

    start = lax.rem(me * WIN, owned)
    row_of = lax.broadcasted_iota(jnp.int32, (WIN, 1), 0) + start
    name = jnp.concatenate([row_of + partner(k) * owned for k in ORDER], axis=0)
    lane = lax.broadcasted_iota(jnp.int32, (1, slots), 1)
    atoms = lax.broadcasted_iota(jnp.int32, (1, LANES), 1)
    matrix[...] = jnp.zeros_like(matrix)

    def scatter(b, carry):
        slot = lax.rem(b, DEPTH)
        ahead = b + DEPTH - 1

        @pl.when(ahead < batches)
        def _():
            fetch(ahead, lax.rem(ahead, DEPTH)).start()

        fetch(b, slot).wait()
        ids = jnp.where(lane < count[b], index[pl.ds(b, 1), :], -1)
        hot = jnp.where(name == ids, 1.0, 0.0).astype(jnp.bfloat16)
        moved = lax.dot_general(hot, held[slot], (((1,), (1,)), ((), ())),
                                preferred_element_type=jnp.float32)
        spread[b] = moved.astype(jnp.bfloat16)
        member[pl.ds(b, 1), :] = jnp.where(atoms == atom[b], 1.0, 0.0)
        return carry

    def group_rows(g):
        return slice(g * LANES, (g + 1) * LANES)

    spots = {}
    for owner in range(cols):
        for e, (i, js) in enumerate(kept[owner]):
            for h, j in enumerate(js):
                spots[i, j] = (owner, 2 * e + h)
    ids_of = {block: n for n, block in enumerate(spots)}

    def block_copy(block):
        owner, slot = spots[block]
        n = ids_of[block]
        return pltpu.make_async_remote_copy(
            src_ref=code.at[n], dst_ref=taken.at[mine, slot],
            send_sem=zsend_sem.at[n], recv_sem=zrecv_sem.at[mine, slot],
            device_id={"col": owner}, device_id_type=MESH)

    def norm_copy(stage, k):
        return pltpu.make_async_remote_copy(
            src_ref=norm.at[stage], dst_ref=norms.at[mine, stage],
            send_sem=vsend_sem.at[stage, k - 1], recv_sem=vrecv_sem.at[mine, stage],
            device_id={"col": lax.rem(mine + k, cols)}, device_id_type=MESH)

    def correlate(stage, fresh):
        tile_row = lax.broadcasted_iota(jnp.int32, (8, LANES), 0)
        tile = jnp.zeros((8, LANES), jnp.float32)
        for g in fresh:
            wide = window[group_rows(g), :].astype(jnp.float32)
            scaled = wide * occ[...]
            high = scaled.astype(jnp.bfloat16)
            split[g, 0:LANES, :] = high
            split[g, LANES:2 * LANES, :] = (scaled - high.astype(jnp.float32)).astype(jnp.bfloat16)
            square = jnp.sum(scaled * wide, axis=1, keepdims=True)
            root = jnp.where(square > 0.0, lax.rsqrt(square), 0.0)
            inverse = jnp.broadcast_to(root * (1.0 / MARGIN), (LANES, LANES))
            scale_col[g] = inverse
            scale_row[g] = inverse.T[0:8, :]
            length = jnp.broadcast_to(square * root * MARGIN, (LANES, LANES)).T
            tile = jnp.where(tile_row == g, length[0:8, :], tile)
        norm[stage] = tile
        for k in range(1, cols):
            norm_copy(stage, k).start()
        for block, (owner, slot) in spots.items():
            i, j = block
            if max(block) not in fresh:
                continue
            both = lax.dot_general(split[j], window[group_rows(i), :], (((1,), (1,)), ((), ())),
                                   preferred_element_type=jnp.float32)
            value = both[0:LANES, :] + both[LANES:2 * LANES, :]
            local[ids_of[block]] = value
            ratio = value * scale_col[j] * scale_row[i, 0:1, :]
            steps = jnp.round(ratio * STEPS).astype(jnp.int32)
            half = LANES // 2
            code[ids_of[block]] = (steps[0:half, :] << 16) | (steps[half:, :] & 0xFFFF)

            @pl.when(mine != owner)
            def _():
                block_copy(block).start()

    def collect(owner, es):
        others = [s for s in range(cols) if s != owner]
        for e in es:
            i, js = kept[owner][e]
            for h, j in enumerate(js):
                slot = 2 * e + h
                value = local[ids_of[i, j]]
                for s in others:
                    pltpu.make_async_remote_copy(
                        src_ref=code.at[0], dst_ref=taken.at[s, slot],
                        send_sem=zsend_sem.at[0], recv_sem=zrecv_sem.at[s, slot],
                        device_id={"col": s}, device_id_type=MESH).wait_recv()
                    word = taken[s, slot]
                    steps = jnp.concatenate([word >> 16, (word << 16) >> 16], axis=0)
                    down = norms[s, stage_of(j), j:j + 1, :] * (1.0 / STEPS)
                    down = jnp.broadcast_to(down, (LANES, LANES)).T
                    value = value + steps.astype(jnp.float32) * down * norms[s, stage_of(i), i:i + 1, :]
                if i != j:
                    value = value + value
                high = value.astype(jnp.bfloat16)
                low = (value - high.astype(jnp.float32)).astype(jnp.bfloat16)
                matrix[e, group_rows(h), 0:LANES] = high
                matrix[e, group_rows(h), LANES:2 * LANES] = low

    needs = [-(-(g + 1) * LANES // WIN) for g in range(groups)]
    stages = [[0, 1, 2]] + [[g] for g in range(3, groups)]

    def stage_of(g):
        return next(n for n, fresh in enumerate(stages) if g in fresh)

    def await_norms(owner, which):
        for stage in which:
            for s in range(cols):
                if s != owner:
                    pltpu.make_async_remote_copy(
                        src_ref=norm.at[stage], dst_ref=norms.at[s, stage],
                        send_sem=vsend_sem.at[stage, 0], recv_sem=vrecv_sem.at[s, stage],
                        device_id={"col": s}, device_id_type=MESH).wait_recv()

    bounds = [batches * n // 40 for n in (0, 16, 26, 36, 40)]
    arrived = 1
    own.wait()
    for stage, fresh in enumerate(stages):
        lax.fori_loop(bounds[stage], bounds[stage + 1], scatter, 0)
        while arrived < needs[fresh[-1]]:
            sends[arrived - 1].wait_recv()
            arrived += 1
        correlate(stage, fresh)

    def chosen(values):
        total = values[0]
        for c in range(1, cols):
            total = jnp.where(mine == c, values[c], total)
        return total

    def group_of(b, g):
        return spread[b, pl.ds(pl.multiple_of(g * LANES, LANES), LANES), :]

    def multiply(b, es):
        total = jnp.zeros((8, points), jnp.float32)
        for e in es:
            i = chosen([kept[c][e][0] for c in range(cols)])
            right = group_of(b, i)
            product = lax.dot_general(matrix[e], jnp.concatenate([right, right], axis=0),
                                      (((1,), (0,)), ((), ())), preferred_element_type=jnp.float32)
            for h in range(2):
                j = chosen([kept[c][e][1][min(h, len(kept[c][e][1]) - 1)] for c in range(cols)])
                term = product[group_rows(h), :] * group_of(b, j).astype(jnp.float32)
                total = total + jnp.sum(term.reshape(LANES // 8, 8, points), axis=0)
        return jnp.sum(total, axis=0, keepdims=True)

    last = len(stages) - 1
    for owner in range(cols):
        @pl.when(mine == owner)
        def _():
            await_norms(owner, range(last))
            collect(owner, range(entries - 1))

    unroll = 4

    def early(step, carry):
        for u in range(unroll):
            b = step * unroll + u
            line[pl.ds(b, 1), :] = multiply(b, range(entries - 1))
        return carry

    lax.fori_loop(0, batches // unroll, early, 0)

    for owner in range(cols):
        @pl.when(mine == owner)
        def _():
            await_norms(owner, [last])
            collect(owner, [entries - 1])

    load.wait()
    moment[...] = jnp.zeros_like(moment)

    def late(step, carry):
        for u in range(8):
            b = step * 8 + u
            line[pl.ds(b, 1), :] += multiply(b, [entries - 1])
        here = pl.ds(pl.multiple_of(step * 8, 8), 8)
        values = line[here, :]
        for c in range(cols):
            dens[c, here, :] = values[:, c * share:(c + 1) * share]
        part = jnp.sum(angular[:, here, :] * values[None], axis=2, keepdims=True)
        moment[...] += jnp.sum(part * member[here, :][None], axis=1)
        return carry

    lax.fori_loop(0, batches // 8, late, 0)

    def exchange(axis, place, size, src_of, dst_of, sent, received):
        copies = []
        for k in range(1, size):
            peer = lax.rem(place + k, size)
            copy = pltpu.make_async_remote_copy(
                src_ref=src_of(peer), dst_ref=dst_of(k),
                send_sem=sent.at[k - 1], recv_sem=received.at[k - 1],
                device_id={axis: peer}, device_id_type=MESH)
            copy.start()
            copies.append(copy)
        return copies

    moved = exchange("col", mine, cols, lambda peer: moment, lambda k: near.at[mine],
                     nsend_sem, nrecv_sem)
    copies = exchange("col", mine, cols, lambda peer: dens.at[peer], lambda k: got.at[k - 1],
                      dsend_sem, drecv_sem)
    near[mine] = moment[...]
    for copy in sends:
        copy.wait_send()
    for stage in range(len(stages)):
        for k in range(1, cols):
            norm_copy(stage, k).wait_send()
    for block, (owner, slot) in spots.items():
        @pl.when(mine != owner)
        def _():
            block_copy(block).wait_send()
    for copy in moved:
        copy.wait()
    total = near[0]
    for c in range(1, cols):
        total = total + near[c]
    moment[...] = total
    far[me] = total
    moved = exchange("row", me, rows, lambda peer: moment, lambda k: far.at[me],
                     fsend_sem, frecv_sem)
    result = dens[mine]
    for k, copy in enumerate(copies):
        copy.wait()
        result = result + got[k]
    out[...] = result
    for copy in moved:
        copy.wait()
    total = far[0]
    for r in range(1, rows):
        total = total + far[r]
    out_moments[...] = total[:, :NATOM]


def fused(coeffs, occupation, basis_on_grid, basis_map, basis_count, batch_atom, harmonics):
    batches, points, slots = basis_on_grid.shape
    owned, states = coeffs.shape
    rows, cols = lax.axis_size("row"), lax.axis_size("col")
    reach = rows * WIN
    groups = reach // LANES
    kept = plan(groups, cols)
    entries = len(kept[0])
    blocks = groups * (groups + 1) // 2
    stages = groups - 2
    vmem, dma = pltpu.VMEM, pltpu.SemaphoreType.DMA
    half, single, word = jnp.bfloat16, jnp.float32, jnp.int32
    whole = pl.BlockSpec(memory_space=pltpu.VMEM)
    scalar = pl.BlockSpec(memory_space=pltpu.SMEM)
    lm = harmonics.shape[1]
    apart = pl.BlockSpec(memory_space=pl.ANY)
    density, moments = pl.pallas_call(
        functools.partial(kernel, rows, cols, owned),
        out_shape=(jax.ShapeDtypeStruct((batches, points // cols), single),
                   jax.ShapeDtypeStruct((lm, NATOM), single)),
        in_specs=[apart, whole, apart, whole, scalar, scalar, apart],
        out_specs=(whole, whole),
        scratch_shapes=[
            vmem((DEPTH, points, slots), half),
            vmem((reach, states), half),
            vmem((groups, 2 * LANES, states), half),
            vmem((blocks, LANES, LANES), single),
            vmem((groups, LANES, LANES), single),
            vmem((groups, 8, LANES), single),
            vmem((stages, 8, LANES), single),
            vmem((blocks, LANES // 2, LANES), word),
            vmem((cols, 2 * entries, LANES // 2, LANES), word),
            vmem((cols, stages, 8, LANES), single),
            vmem((entries, 2 * LANES, 2 * LANES), half),
            vmem((batches, reach, points), half),
            vmem((lm, batches, points), single),
            vmem((batches, LANES), single),
            vmem((batches, points), single),
            vmem((cols, batches, points // cols), single),
            vmem((cols - 1, batches, points // cols), single),
            vmem((cols, lm, LANES), single),
            vmem((rows, lm, LANES), single),
            vmem((lm, LANES), single),
            dma, dma((DEPTH,)), dma, dma((rows - 1,)), dma((rows - 1,)),
            dma((blocks,)), dma((cols, 2 * entries)), dma((stages, cols - 1)), dma((cols, stages)),
            dma((cols - 1,)), dma((cols - 1,)), dma((cols - 1,)), dma((cols - 1,)),
            dma((rows - 1,)), dma((rows - 1,)),
        ],
        compiler_params=pltpu.CompilerParams(
            collective_id=0, has_side_effects=True, vmem_limit_bytes=VMEM_BYTES),
    )(coeffs, occupation.reshape(1, -1), basis_on_grid, basis_map, basis_count,
      batch_atom, jnp.transpose(harmonics, (1, 0, 2)))
    return density, moments.T


def shards(coeffs, occupation, basis_on_grid, basis_map, basis_count, batch_atom, harmonics):
    batches, points, slots = basis_on_grid.shape
    owned, states = coeffs.shape
    rows, cols = lax.axis_size("row"), lax.axis_size("col")
    reach = rows * WIN
    share = points // cols
    needed = batches * reach * points * 2 + 10 * reach * states
    fits = needed < VMEM_BYTES * 3 // 4 and share % LANES == 0 and owned % WIN == 0
    if fits and rows == len(ORDER) and cols == 4 and reach % LANES == 0 and batches % 8 == 0:
        return fused(coeffs, occupation, basis_on_grid, basis_map, basis_count,
                     batch_atom, harmonics)
    density = plain(coeffs, occupation, basis_on_grid, basis_map, basis_count)
    part = lax.dynamic_slice_in_dim(harmonics, lax.axis_index("col") * share, share, 2)
    local_moment = jnp.sum(part * density[:, None, :], axis=2)
    atom_ids = lax.broadcasted_iota(jnp.int32, (batches, NATOM), 1)
    member = (batch_atom[:, None] == atom_ids).astype(jnp.float32)
    atom_part = jnp.dot(member.T, local_moment, precision=lax.Precision.HIGHEST)
    moments = lax.psum(atom_part, ("row", "col"))
    return (density, moments)


def solution(mesh):
    placed = (
        P("row", "col"),
        P("col"),
        P("row", None, None),
        P("row", None),
        P("row"),
        P("row"),
        P("row", None, None),
    )
    return jax.shard_map(
        shards, mesh=mesh, in_specs=placed, out_specs=(P("row", "col"), P()), check_vma=False
    )
```

```python
import functools

import jax
import jax.numpy as jnp
from jax import lax
from jax.experimental import pallas as pl
from jax.experimental.pallas import tpu as pltpu
from jax.sharding import PartitionSpec as P

WIN = 96
NATOM = 64
LANES = 128
VMEM_BYTES = 62 * 1024 * 1024
STEP = 4
DEPTH = 2 * STEP
STEPS = 32767.0
MARGIN = 1.0 + 2.0 ** -7
MESH = pl.DeviceIdType.MESH
ORDER = (0, 1, 2, 4, 3, 5, 6, 7)
KEPT = (
    ((0, (2, 3)), (1, (2, 3)), (1, (1,))),
    ((4, (0, 1)), (0, (0, 1)), (5, (0, 1))),
    ((4, (2, 3)), (2, (2, 3)), (5, (2, 3))),
    ((3, (3,)), (4, (4,)), (5, (4, 5))),
)
USED = ((0, 1, 2, 3), (0, 1, 4, 5), (2, 3, 4, 5), (2, 3, 4, 5))


def plain(coeffs, occupation, basis_on_grid, basis_map, basis_count):
    batches, points, slots = basis_on_grid.shape
    owned = coeffs.shape[0]
    owners = lax.axis_size("row")
    target = lax.broadcasted_iota(jnp.int32, (owners, WIN), 0)
    offset = lax.broadcasted_iota(jnp.int32, (owners, WIN), 1)
    outgoing_ids = jnp.mod(target * WIN + offset, owned).reshape(-1)
    outgoing = jnp.take(coeffs, outgoing_ids, axis=0)
    window = lax.all_to_all(outgoing, "row", split_axis=0, concat_axis=0, tiled=True)
    start = jnp.mod(lax.axis_index("row") * WIN, owned)
    source = basis_map // owned
    within = jnp.mod(basis_map % owned - start, owned)
    local_ids = source * WIN + within
    selected = jnp.take(window, local_ids, axis=0)
    slot_ids = lax.broadcasted_iota(jnp.int32, (batches, slots), 1)
    keep = slot_ids < basis_count[:, None]
    masked = jnp.where(keep[:, None, :], basis_on_grid, jnp.zeros_like(basis_on_grid))
    orbital = jnp.einsum("bps,bsk->bpk", masked, selected, preferred_element_type=jnp.float32)
    partial_density = jnp.sum(orbital * orbital * occupation[None, None, :], axis=2)
    full_density = lax.psum(partial_density, "col")
    share = points // lax.axis_size("col")
    return lax.dynamic_slice_in_dim(full_density, lax.axis_index("col") * share, share, 1)


def kernel(rows, cols, owned, coeffs, occ, basis, index, count, atom, harmonics, out, out_moments,
           held, names, window, split, local, scale_col, scale_row, norm, code, taken, norms, matrix,
           spread, angular, member, line, dens, got, near, far, moment,
           own_sem, in_sem, angular_sem, send_sem, recv_sem, zsend_sem, zrecv_sem, vsend_sem, vrecv_sem,
           dsend_sem, drecv_sem, nsend_sem, nrecv_sem, fsend_sem, frecv_sem):
    batches, points, slots = basis.shape
    states = coeffs.shape[1]
    reach = rows * WIN
    groups = reach // LANES
    me, mine = lax.axis_index("row"), lax.axis_index("col")
    share = points // cols
    kept, entries = KEPT, len(KEPT[0])

    barrier = pltpu.get_barrier_semaphore()
    for k in range(1, rows):
        pl.semaphore_signal(barrier, inc=1, device_id={"row": lax.rem(me + k, rows)},
                            device_id_type=MESH)
    for k in range(1, cols):
        pl.semaphore_signal(barrier, inc=1, device_id={"col": lax.rem(mine + k, cols)},
                            device_id_type=MESH)

    def fetch(b, slot):
        return pltpu.make_async_copy(basis.at[b], held.at[slot], in_sem.at[slot])

    for b in range(STEP):
        fetch(b, b).start()

    def chosen(values):
        total = values[0]
        for c in range(1, cols):
            total = jnp.where(mine == c, values[c], total)
        return total

    def rows_for(owner):
        return coeffs.at[pl.ds(pl.multiple_of(lax.rem(owner * WIN, owned), 32), WIN), :]

    def partner(k):
        bits = (lax.rem(me, 2), lax.rem(lax.div(me, 2), 2), lax.div(me, 4))
        return sum((1 - bit if k >> n & 1 else bit) * (1 << n) for n, bit in enumerate(bits))

    own = pltpu.make_async_copy(rows_for(me), window.at[0:WIN, :], own_sem)
    own.start()
    pl.semaphore_wait(barrier, rows + cols - 2)
    sends = []
    for p in range(1, rows):
        peer = partner(ORDER[p])
        copy = pltpu.make_async_remote_copy(
            src_ref=rows_for(peer), dst_ref=window.at[p * WIN:(p + 1) * WIN, :],
            send_sem=send_sem.at[p - 1], recv_sem=recv_sem.at[p - 1],
            device_id={"row": peer}, device_id_type=MESH)
        copy.start()
        sends.append(copy)
    load = pltpu.make_async_copy(harmonics, angular, angular_sem)
    load.start()

    start = lax.rem(me * WIN, owned)
    for r in range(len(USED[0])):
        row = lax.broadcasted_iota(jnp.int32, (LANES, LANES), 0) + chosen([g[r] for g in USED]) * LANES
        found = jnp.zeros_like(row)
        for p, k in enumerate(ORDER):
            own_row = row - p * WIN
            found = jnp.where((own_row >= 0) & (own_row < WIN), own_row + (start + partner(k) * owned), found)
        names[r * LANES:(r + 1) * LANES, :] = found
    lane = lax.broadcasted_iota(jnp.int32, (1, slots), 1)
    atoms = lax.broadcasted_iota(jnp.int32, (1, LANES), 1)
    matrix[...] = jnp.zeros_like(matrix)

    def scatter(step, carry):
        first = step * STEP
        base = lax.rem(step, 2) * STEP

        @pl.when(first + STEP < batches)
        def _():
            for u in range(STEP):
                fetch(first + STEP + u, STEP - base + u).start()

        for u in range(STEP):
            fetch(first + u, base + u).wait()
        for u in range(STEP):
            b = first + u
            ids = jnp.where(lane < count[b], index[pl.ds(b, 1), :], -1)
            hot = jnp.concatenate(
                [jnp.where(names[...] == ids[:, n:n + LANES], 1.0, 0.0) for n in range(0, slots, LANES)],
                axis=1).astype(jnp.bfloat16)
            moved = lax.dot_general(hot, held[base + u], (((1,), (1,)), ((), ())),
                                    preferred_element_type=jnp.float32)
            spread[b] = moved.astype(jnp.bfloat16)
            member[pl.ds(b, 1), :] = jnp.where(lax.rem(atoms, NATOM) == atom[b], 1.0, 0.0)
        return carry

    def group_rows(g):
        return slice(g * LANES, (g + 1) * LANES)

    spots = {}
    for owner in range(cols):
        for e, (i, js) in enumerate(kept[owner]):
            for h, j in enumerate(js):
                spots[i, j] = (owner, 2 * e + h)
    ids_of = {block: n for n, block in enumerate(spots)}

    def block_copy(block):
        owner, slot = spots[block]
        n = ids_of[block]
        return pltpu.make_async_remote_copy(
            src_ref=code.at[n], dst_ref=taken.at[mine, slot],
            send_sem=zsend_sem.at[n], recv_sem=zrecv_sem.at[mine, slot],
            device_id={"col": owner}, device_id_type=MESH)

    def norm_copy(stage, k):
        return pltpu.make_async_remote_copy(
            src_ref=norm.at[stage], dst_ref=norms.at[mine, stage],
            send_sem=vsend_sem.at[stage, k - 1], recv_sem=vrecv_sem.at[mine, stage],
            device_id={"col": lax.rem(mine + k, cols)}, device_id_type=MESH)

    def correlate(stage, fresh):
        tile_row = lax.broadcasted_iota(jnp.int32, (8, LANES), 0)
        tile = jnp.zeros((8, LANES), jnp.float32)
        for g in fresh:
            wide = window[group_rows(g), :].astype(jnp.float32)
            scaled = wide * occ[...]
            high = scaled.astype(jnp.bfloat16)
            split[g, 0:LANES, :] = high
            split[g, LANES:2 * LANES, :] = (scaled - high.astype(jnp.float32)).astype(jnp.bfloat16)
            square = jnp.sum(scaled * wide, axis=1, keepdims=True)
            root = jnp.where(square > 0.0, lax.rsqrt(square), 0.0)
            inverse = jnp.broadcast_to(root * (1.0 / MARGIN), (LANES, LANES))
            scale_col[g] = inverse
            scale_row[g] = inverse.T[0:8, :]
            length = jnp.broadcast_to(square * root * MARGIN, (LANES, LANES)).T
            tile = jnp.where(tile_row == g, length[0:8, :], tile)
        norm[stage] = tile
        for k in range(1, cols):
            norm_copy(stage, k).start()
        made = {}
        for j in fresh:
            for first in range(0, j + 1, 2):
                lanes = range(first, min(first + 2, j + 1))
                right = window[first * LANES:(lanes[-1] + 1) * LANES, :]
                both = lax.dot_general(split[j], right, (((1,), (1,)), ((), ())),
                                       preferred_element_type=jnp.float32)
                value = both[0:LANES, :] + both[LANES:2 * LANES, :]
                for n, i in enumerate(lanes):
                    made[i, j] = value[:, group_rows(n)]
        ready = [block for block in spots if max(block) in fresh]
        for i, j in ready:
            value = made[i, j] if i <= j else made[j, i].T
            n = ids_of[i, j]
            local[n] = value
            ratio = value * scale_col[j] * scale_row[i, 0:1, :]
            steps = jnp.round(ratio * STEPS).astype(jnp.int32)
            half = LANES // 2
            code[n] = (steps[0:half, :] << 16) | (steps[half:, :] & 0xFFFF)
        for owner in range(cols):
            @pl.when(mine != owner)
            def _():
                for block in ready:
                    if spots[block][0] == owner:
                        block_copy(block).start()

    def collect(owner, es):
        others = [s for s in range(cols) if s != owner]
        for e in es:
            i, js = kept[owner][e]
            for h, j in enumerate(js):
                slot = 2 * e + h
                value = local[ids_of[i, j]]
                for s in others:
                    pltpu.make_async_remote_copy(
                        src_ref=code.at[0], dst_ref=taken.at[s, slot],
                        send_sem=zsend_sem.at[0], recv_sem=zrecv_sem.at[s, slot],
                        device_id={"col": s}, device_id_type=MESH).wait_recv()
                    word = taken[s, slot]
                    steps = jnp.concatenate([word >> 16, (word << 16) >> 16], axis=0)
                    down = norms[s, stage_of(j), j:j + 1, :] * (1.0 / STEPS)
                    down = jnp.broadcast_to(down, (LANES, LANES)).T
                    value = value + steps.astype(jnp.float32) * down * norms[s, stage_of(i), i:i + 1, :]
                if i != j:
                    value = value + value
                high = value.astype(jnp.bfloat16)
                low = (value - high.astype(jnp.float32)).astype(jnp.bfloat16)
                matrix[e, group_rows(h), 0:LANES] = high
                matrix[e, group_rows(h), LANES:2 * LANES] = low

    needs = [-(-(g + 1) * LANES // WIN) for g in range(groups)]
    stages = [[0, 1, 2]] + [[g] for g in range(3, groups)]

    def stage_of(g):
        return next(n for n, fresh in enumerate(stages) if g in fresh)

    def await_norms(owner, which):
        for stage in which:
            for s in range(cols):
                if s != owner:
                    pltpu.make_async_remote_copy(
                        src_ref=norm.at[stage], dst_ref=norms.at[s, stage],
                        send_sem=vsend_sem.at[stage, 0], recv_sem=vrecv_sem.at[s, stage],
                        device_id={"col": s}, device_id_type=MESH).wait_recv()

    bounds = [batches // STEP * n // 10 for n in (0, 4, 6, 8, 10)]
    arrived = 1
    own.wait()
    for stage, fresh in enumerate(stages):
        lax.fori_loop(bounds[stage], bounds[stage + 1], scatter, 0)
        while arrived < needs[fresh[-1]]:
            sends[arrived - 1].wait_recv()
            arrived += 1
        correlate(stage, fresh)

    def group_of(b, g):
        return spread[b, pl.ds(pl.multiple_of(g * LANES, LANES), LANES), :]

    def multiply(b, es):
        total = jnp.zeros((8, points), jnp.float32)
        for e in es:
            i = chosen([USED[c].index(kept[c][e][0]) for c in range(cols)])
            right = group_of(b, i)
            product = lax.dot_general(matrix[e], jnp.concatenate([right, right], axis=0),
                                      (((1,), (0,)), ((), ())), preferred_element_type=jnp.float32)
            for h in range(2):
                j = chosen([USED[c].index(kept[c][e][1][min(h, len(kept[c][e][1]) - 1)]) for c in range(cols)])
                term = product[group_rows(h), :] * group_of(b, j).astype(jnp.float32)
                total = total + jnp.sum(term.reshape(LANES // 8, 8, points), axis=0)
        return jnp.sum(total, axis=0, keepdims=True)

    last = len(stages) - 1
    for owner in range(cols):
        @pl.when(mine == owner)
        def _():
            await_norms(owner, range(last))
            collect(owner, range(entries - 1))

    unroll = 4

    def early(step, carry):
        for u in range(unroll):
            b = step * unroll + u
            line[pl.ds(b, 1), :] = multiply(b, range(entries - 1))
        return carry

    lax.fori_loop(0, batches // unroll, early, 0)

    for owner in range(cols):
        @pl.when(mine == owner)
        def _():
            await_norms(owner, [last])
            collect(owner, [entries - 1])

    load.wait()
    moment[...] = jnp.zeros_like(moment)

    def late(step, carry):
        for u in range(8):
            b = step * 8 + u
            line[pl.ds(b, 1), :] += multiply(b, [entries - 1])
        here = pl.ds(pl.multiple_of(step * 8, 8), 8)
        values = line[here, :]
        for c in range(cols):
            dens[c, here, :] = values[:, c * share:(c + 1) * share]
        part = jnp.sum(angular[:, here, :] * values[None], axis=2, keepdims=True)
        packed = moment.shape[0]
        low, high = part[:packed], part[part.shape[0] - packed:]
        moment[...] += jnp.sum(jnp.where(atoms[None] < NATOM, low, high) * member[here, :][None], axis=1)
        return carry

    lax.fori_loop(0, batches // 8, late, 0)

    def exchange(axis, place, size, src_of, dst_of, sent, received):
        copies = []
        for k in range(1, size):
            peer = lax.rem(place + k, size)
            copy = pltpu.make_async_remote_copy(
                src_ref=src_of(peer), dst_ref=dst_of(k),
                send_sem=sent.at[k - 1], recv_sem=received.at[k - 1],
                device_id={axis: peer}, device_id_type=MESH)
            copy.start()
            copies.append(copy)
        return copies

    moved = exchange("col", mine, cols, lambda peer: moment, lambda k: near.at[mine],
                     nsend_sem, nrecv_sem)
    copies = exchange("col", mine, cols, lambda peer: dens.at[peer], lambda k: got.at[k - 1],
                      dsend_sem, drecv_sem)
    near[mine] = moment[...]
    for copy in sends:
        copy.wait_send()
    for stage in range(len(stages)):
        for k in range(1, cols):
            norm_copy(stage, k).wait_send()
    for owner in range(cols):
        @pl.when(mine != owner)
        def _():
            for block in spots:
                if spots[block][0] == owner:
                    block_copy(block).wait_send()
    for copy in moved:
        copy.wait()
    total = near[0]
    for c in range(1, cols):
        total = total + near[c]
    moment[...] = total
    far[me] = total
    moved = exchange("row", me, rows, lambda peer: moment, lambda k: far.at[me],
                     fsend_sem, frecv_sem)
    result = dens[mine]
    for k, copy in enumerate(copies):
        copy.wait()
        result = result + got[k]
    out[...] = result
    for copy in moved:
        copy.wait()
    total = far[0]
    for r in range(1, rows):
        total = total + far[r]
    out_moments[...] = total


def finish(density, moments, out, out_moments):
    out[...] = density[...]
    packed, lm = moments.shape[0], out_moments.shape[0]
    out_moments[lm - packed:, :] = moments[:, NATOM:]
    out_moments[:packed, :] = moments[:, :NATOM]


def fused(coeffs, occupation, basis_on_grid, basis_map, basis_count, batch_atom, harmonics):
    batches, points, slots = basis_on_grid.shape
    owned, states = coeffs.shape
    rows, cols = lax.axis_size("row"), lax.axis_size("col")
    reach = rows * WIN
    groups = reach // LANES
    entries = len(KEPT[0])
    blocks = groups * (groups + 1) // 2
    stages = groups - 2
    vmem, dma = pltpu.VMEM, pltpu.SemaphoreType.DMA
    half, single, word = jnp.bfloat16, jnp.float32, jnp.int32
    whole = pl.BlockSpec(memory_space=pltpu.VMEM)
    scalar = pl.BlockSpec(memory_space=pltpu.SMEM)
    lm = harmonics.shape[1]
    packed = (lm + 1) // 2
    apart = pl.BlockSpec(memory_space=pl.ANY)
    density, moments = pl.pallas_call(
        functools.partial(kernel, rows, cols, owned),
        out_shape=(jax.ShapeDtypeStruct((batches, points // cols), single),
                   jax.ShapeDtypeStruct((packed, LANES), single)),
        in_specs=[apart, whole, apart, whole, scalar, scalar, apart],
        out_specs=(whole, whole),
        scratch_shapes=[
            vmem((DEPTH, points, slots), half),
            vmem((len(USED[0]) * LANES, LANES), word),
            vmem((reach, states), half),
            vmem((groups, 2 * LANES, states), half),
            vmem((blocks, LANES, LANES), single),
            vmem((groups, LANES, LANES), single),
            vmem((groups, 8, LANES), single),
            vmem((stages, 8, LANES), single),
            vmem((blocks, LANES // 2, LANES), word),
            vmem((cols, 2 * entries, LANES // 2, LANES), word),
            vmem((cols, stages, 8, LANES), single),
            vmem((entries, 2 * LANES, 2 * LANES), half),
            vmem((batches, len(USED[0]) * LANES, points), half),
            vmem((lm, batches, points), single),
            vmem((batches, LANES), single),
            vmem((batches, points), single),
            vmem((cols, batches, points // cols), single),
            vmem((cols - 1, batches, points // cols), single),
            vmem((cols, packed, LANES), single),
            vmem((rows, packed, LANES), single),
            vmem((packed, LANES), single),
            dma, dma((DEPTH,)), dma, dma((rows - 1,)), dma((rows - 1,)),
            dma((blocks,)), dma((cols, 2 * entries)), dma((stages, cols - 1)), dma((cols, stages)),
            dma((cols - 1,)), dma((cols - 1,)), dma((cols - 1,)), dma((cols - 1,)),
            dma((rows - 1,)), dma((rows - 1,)),
        ],
        compiler_params=pltpu.CompilerParams(
            collective_id=0, has_side_effects=True, vmem_limit_bytes=VMEM_BYTES),
    )(coeffs, occupation.reshape(1, -1), basis_on_grid, basis_map, basis_count,
      batch_atom, jnp.transpose(harmonics, (1, 0, 2)))
    density, moments = pl.pallas_call(
        finish, out_shape=(jax.ShapeDtypeStruct(density.shape, single),
                           jax.ShapeDtypeStruct((lm, NATOM), single)),
        in_specs=[whole, whole], out_specs=(whole, whole))(density, moments)
    return density, moments.T


def shards(coeffs, occupation, basis_on_grid, basis_map, basis_count, batch_atom, harmonics):
    batches, points, slots = basis_on_grid.shape
    owned, states = coeffs.shape
    rows, cols = lax.axis_size("row"), lax.axis_size("col")
    reach = rows * WIN
    share = points // cols
    needed = batches * reach * points * 2 + 10 * reach * states
    fits = needed < VMEM_BYTES * 3 // 4 and share % LANES == 0 and owned % WIN == 0
    if fits and rows == len(ORDER) and cols == len(KEPT) and reach == 6 * LANES and 2 * NATOM == LANES and batches % (2 * STEP) == 0:
        return fused(coeffs, occupation, basis_on_grid, basis_map, basis_count,
                     batch_atom, harmonics)
    density = plain(coeffs, occupation, basis_on_grid, basis_map, basis_count)
    part = lax.dynamic_slice_in_dim(harmonics, lax.axis_index("col") * share, share, 2)
    local_moment = jnp.sum(part * density[:, None, :], axis=2)
    atom_ids = lax.broadcasted_iota(jnp.int32, (batches, NATOM), 1)
    member = (batch_atom[:, None] == atom_ids).astype(jnp.float32)
    atom_part = jnp.dot(member.T, local_moment, precision=lax.Precision.HIGHEST)
    moments = lax.psum(atom_part, ("row", "col"))
    return (density, moments)


def solution(mesh):
    placed = (
        P("row", "col"),
        P("col"),
        P("row", None, None),
        P("row", None),
        P("row"),
        P("row"),
        P("row", None, None),
    )
    return jax.shard_map(
        shards, mesh=mesh, in_specs=placed, out_specs=(P("row", "col"), P()), check_vma=False
    )
```

```python
import functools

import jax
import jax.numpy as jnp
from jax import lax
from jax.experimental import pallas as pl
from jax.experimental.pallas import tpu as pltpu
from jax.sharding import PartitionSpec as P

WIN = 96
NATOM = 64
LANES = 128
VMEM_BYTES = 62 * 1024 * 1024
STEP = 4
DEPTH = 2 * STEP
STEPS = 32767.0
MARGIN = 1.0 + 2.0 ** -7
MESH = pl.DeviceIdType.MESH
ORDER = (0, 1, 2, 4, 3, 5, 6, 7)
KEPT = (
    ((0, (2, 3)), (1, (2, 3)), (1, (1,))),
    ((0, (0, 1)), (4, (0, 1)), (5, (0, 1))),
    ((2, (2, 3)), (4, (2, 3)), (5, (2, 3))),
    ((3, (3,)), (4, (4,)), (5, (4, 5))),
)
USED = ((0, 1, 2, 3), (0, 1, 4, 5), (2, 3, 4, 5), (2, 3, 4, 5))


def plain(coeffs, occupation, basis_on_grid, basis_map, basis_count):
    batches, points, slots = basis_on_grid.shape
    owned = coeffs.shape[0]
    owners = lax.axis_size("row")
    target = lax.broadcasted_iota(jnp.int32, (owners, WIN), 0)
    offset = lax.broadcasted_iota(jnp.int32, (owners, WIN), 1)
    outgoing_ids = jnp.mod(target * WIN + offset, owned).reshape(-1)
    outgoing = jnp.take(coeffs, outgoing_ids, axis=0)
    window = lax.all_to_all(outgoing, "row", split_axis=0, concat_axis=0, tiled=True)
    start = jnp.mod(lax.axis_index("row") * WIN, owned)
    source = basis_map // owned
    within = jnp.mod(basis_map % owned - start, owned)
    local_ids = source * WIN + within
    selected = jnp.take(window, local_ids, axis=0)
    slot_ids = lax.broadcasted_iota(jnp.int32, (batches, slots), 1)
    keep = slot_ids < basis_count[:, None]
    masked = jnp.where(keep[:, None, :], basis_on_grid, jnp.zeros_like(basis_on_grid))
    orbital = jnp.einsum("bps,bsk->bpk", masked, selected, preferred_element_type=jnp.float32)
    partial_density = jnp.sum(orbital * orbital * occupation[None, None, :], axis=2)
    full_density = lax.psum(partial_density, "col")
    share = points // lax.axis_size("col")
    return lax.dynamic_slice_in_dim(full_density, lax.axis_index("col") * share, share, 1)


def kernel(rows, cols, owned, coeffs, occ_in, basis, index_in, count_in, atom_in, harmonics, out, out_moments,
           occ, index, count, atom, held, names, window, split, local, scale_col, scale_row, norm, code, taken, norms, matrix,
           spread, angular, member, line, dens, got, near, far, moment,
           small_sem, own_sem, in_sem, angular_sem, send_sem, recv_sem, zsend_sem, zrecv_sem, vsend_sem, vrecv_sem,
           dsend_sem, drecv_sem, nsend_sem, nrecv_sem, fsend_sem, frecv_sem):
    batches, points, slots = basis.shape
    states = coeffs.shape[1]
    reach = rows * WIN
    groups = reach // LANES
    me, mine = lax.axis_index("row"), lax.axis_index("col")
    share = points // cols
    kept, entries = KEPT, len(KEPT[0])

    barrier = pltpu.get_barrier_semaphore()
    for k in range(1, rows):
        pl.semaphore_signal(barrier, inc=1, device_id={"row": lax.rem(me + k, rows)},
                            device_id_type=MESH)
    for k in range(1, cols):
        pl.semaphore_signal(barrier, inc=1, device_id={"col": lax.rem(mine + k, cols)},
                            device_id_type=MESH)

    def fetch(b, slot):
        return pltpu.make_async_copy(basis.at[b], held.at[slot], in_sem.at[slot])

    small = [pltpu.make_async_copy(src, dst, small_sem.at[n]) for n, (src, dst) in enumerate(
        ((count_in, count), (index_in, index), (atom_in, atom), (occ_in, occ)))]
    for copy in small:
        copy.start()
    for b in range(STEP):
        fetch(b, b).start()

    def chosen(values):
        total = values[0]
        for c in range(1, cols):
            total = jnp.where(mine == c, values[c], total)
        return total

    def rows_for(owner):
        return coeffs.at[pl.ds(pl.multiple_of(lax.rem(owner * WIN, owned), 32), WIN), :]

    def partner(k):
        bits = (lax.rem(me, 2), lax.rem(lax.div(me, 2), 2), lax.div(me, 4))
        return sum((1 - bit if k >> n & 1 else bit) * (1 << n) for n, bit in enumerate(bits))

    own = pltpu.make_async_copy(rows_for(me), window.at[0:WIN, :], own_sem)
    own.start()
    pl.semaphore_wait(barrier, rows + cols - 2)
    sends = []
    for p in range(1, rows):
        peer = partner(ORDER[p])
        copy = pltpu.make_async_remote_copy(
            src_ref=rows_for(peer), dst_ref=window.at[p * WIN:(p + 1) * WIN, :],
            send_sem=send_sem.at[p - 1], recv_sem=recv_sem.at[p - 1],
            device_id={"row": peer}, device_id_type=MESH)
        copy.start()
        sends.append(copy)
    load = pltpu.make_async_copy(harmonics, angular, angular_sem)
    load.start()

    start = lax.rem(me * WIN, owned)
    for r in range(len(USED[0])):
        row = lax.broadcasted_iota(jnp.int32, (LANES, LANES), 0) + chosen([g[r] for g in USED]) * LANES
        found = jnp.zeros_like(row)
        for p, k in enumerate(ORDER):
            own_row = row - p * WIN
            found = jnp.where((own_row >= 0) & (own_row < WIN), own_row + (start + partner(k) * owned), found)
        names[r * LANES:(r + 1) * LANES, :] = found
    lane = lax.broadcasted_iota(jnp.int32, (1, slots), 1)
    atoms = lax.broadcasted_iota(jnp.int32, (1, LANES), 1)
    matrix[...] = jnp.zeros_like(matrix)

    def scatter(step, carry):
        first = step * STEP
        base = lax.rem(step, 2) * STEP

        @pl.when(first + STEP < batches)
        def _():
            for u in range(STEP):
                fetch(first + STEP + u, STEP - base + u).start()

        for u in range(STEP):
            fetch(first + u, base + u).wait()
        for u in range(STEP):
            b = first + u
            ids = jnp.where(lane < count[b], index[pl.ds(b, 1), :], -1)
            hot = jnp.concatenate(
                [jnp.where(names[...] == ids[:, n:n + LANES], 1.0, 0.0) for n in range(0, slots, LANES)],
                axis=1).astype(jnp.bfloat16)
            moved = lax.dot_general(hot, held[base + u], (((1,), (1,)), ((), ())),
                                    preferred_element_type=jnp.float32)
            spread[b] = moved.astype(jnp.bfloat16)
            member[pl.ds(b, 1), :] = jnp.where(lax.rem(atoms, NATOM) == atom[b], 1.0, 0.0)
        return carry

    def group_rows(g):
        return slice(g * LANES, (g + 1) * LANES)

    spots = {}
    for owner in range(cols):
        for e, (i, js) in enumerate(kept[owner]):
            for h, j in enumerate(js):
                spots[i, j] = (owner, 2 * e + h)
    ids_of = {block: n for n, block in enumerate(spots)}

    def block_copy(block):
        owner, slot = spots[block]
        n = ids_of[block]
        return pltpu.make_async_remote_copy(
            src_ref=code.at[n], dst_ref=taken.at[mine, slot],
            send_sem=zsend_sem.at[n], recv_sem=zrecv_sem.at[mine, slot],
            device_id={"col": owner}, device_id_type=MESH)

    def norm_copy(stage, k):
        return pltpu.make_async_remote_copy(
            src_ref=norm.at[stage], dst_ref=norms.at[mine, stage],
            send_sem=vsend_sem.at[stage, k - 1], recv_sem=vrecv_sem.at[mine, stage],
            device_id={"col": lax.rem(mine + k, cols)}, device_id_type=MESH)

    def correlate(stage, fresh):
        tile_row = lax.broadcasted_iota(jnp.int32, (8, LANES), 0)
        tile = jnp.zeros((8, LANES), jnp.float32)
        for g in fresh:
            wide = window[group_rows(g), :].astype(jnp.float32)
            scaled = wide * occ[...]
            high = scaled.astype(jnp.bfloat16)
            split[g, 0:LANES, :] = high
            split[g, LANES:2 * LANES, :] = (scaled - high.astype(jnp.float32)).astype(jnp.bfloat16)
            square = jnp.sum(scaled * wide, axis=1, keepdims=True)
            root = jnp.where(square > 0.0, lax.rsqrt(square), 0.0)
            inverse = jnp.broadcast_to(root * (1.0 / MARGIN), (LANES, LANES))
            scale_col[g] = inverse
            scale_row[g] = inverse.T[0:8, :]
            length = jnp.broadcast_to(square * root * MARGIN, (LANES, LANES)).T
            tile = jnp.where(tile_row == g, length[0:8, :], tile)
        norm[stage] = tile
        for k in range(1, cols):
            norm_copy(stage, k).start()
        made = {}
        for j in fresh:
            for first in range(0, j + 1, 2):
                lanes = range(first, min(first + 2, j + 1))
                right = window[first * LANES:(lanes[-1] + 1) * LANES, :]
                both = lax.dot_general(split[j], right, (((1,), (1,)), ((), ())),
                                       preferred_element_type=jnp.float32)
                value = both[0:LANES, :] + both[LANES:2 * LANES, :]
                for n, i in enumerate(lanes):
                    made[i, j] = value[:, group_rows(n)]
        ready = [block for block in spots if max(block) in fresh]
        for i, j in ready:
            value = made[i, j] if i <= j else made[j, i].T
            n = ids_of[i, j]
            local[n] = value
            ratio = value * scale_col[j] * scale_row[i, 0:1, :]
            steps = jnp.round(ratio * STEPS).astype(jnp.int32)
            half = LANES // 2
            code[n] = (steps[0:half, :] << 16) | (steps[half:, :] & 0xFFFF)
        for owner in range(cols):
            @pl.when(mine != owner)
            def _():
                for block in ready:
                    if spots[block][0] == owner:
                        block_copy(block).start()

    def collect(owner, es):
        others = [s for s in range(cols) if s != owner]
        for e in es:
            i, js = kept[owner][e]
            for h, j in enumerate(js):
                slot = 2 * e + h
                value = local[ids_of[i, j]]
                for s in others:
                    pltpu.make_async_remote_copy(
                        src_ref=code.at[0], dst_ref=taken.at[s, slot],
                        send_sem=zsend_sem.at[0], recv_sem=zrecv_sem.at[s, slot],
                        device_id={"col": s}, device_id_type=MESH).wait_recv()
                    word = taken[s, slot]
                    steps = jnp.concatenate([word >> 16, (word << 16) >> 16], axis=0)
                    down = norms[s, stage_of(j), j:j + 1, :] * (1.0 / STEPS)
                    down = jnp.broadcast_to(down, (LANES, LANES)).T
                    value = value + steps.astype(jnp.float32) * down * norms[s, stage_of(i), i:i + 1, :]
                if i != j:
                    value = value + value
                high = value.astype(jnp.bfloat16)
                low = (value - high.astype(jnp.float32)).astype(jnp.bfloat16)
                matrix[e, group_rows(h), 0:LANES] = high
                matrix[e, group_rows(h), LANES:2 * LANES] = low

    needs = [-(-(g + 1) * LANES // WIN) for g in range(groups)]
    stages = [[0, 1, 2]] + [[g] for g in range(3, groups)]

    def stage_of(g):
        return next(n for n, fresh in enumerate(stages) if g in fresh)

    def await_norms(owner, which):
        for stage in which:
            for s in range(cols):
                if s != owner:
                    pltpu.make_async_remote_copy(
                        src_ref=norm.at[stage], dst_ref=norms.at[s, stage],
                        send_sem=vsend_sem.at[stage, 0], recv_sem=vrecv_sem.at[s, stage],
                        device_id={"col": s}, device_id_type=MESH).wait_recv()

    def group_of(b, g):
        return spread[b, pl.ds(pl.multiple_of(g * LANES, LANES), LANES), :]

    def multiply(b, es):
        total = jnp.zeros((8, points), jnp.float32)
        for e in es:
            i = chosen([USED[c].index(kept[c][e][0]) for c in range(cols)])
            right = group_of(b, i)
            product = lax.dot_general(matrix[e], jnp.concatenate([right, right], axis=0),
                                      (((1,), (0,)), ((), ())), preferred_element_type=jnp.float32)
            for h in range(2):
                j = chosen([USED[c].index(kept[c][e][1][min(h, len(kept[c][e][1]) - 1)]) for c in range(cols)])
                term = product[group_rows(h), :] * group_of(b, j).astype(jnp.float32)
                total = total + jnp.sum(term.reshape(LANES // 8, 8, points), axis=0)
        return jnp.sum(total, axis=0, keepdims=True)

    def take(e, which):
        for owner in range(cols):
            @pl.when(mine == owner)
            def _():
                await_norms(owner, which)
                collect(owner, [e])

    def add(e):
        def body(step, carry):
            for u in range(8):
                b = step * 8 + u
                value = multiply(b, [e])
                line[pl.ds(b, 1), :] = value if e == 0 else line[pl.ds(b, 1), :] + value
            return carry

        lax.fori_loop(0, batches // 8, body, 0)

    last = len(stages) - 1
    bounds = [batches // STEP * n // 10 for n in (0, 4, 7, 10, 10)]
    arrived = 1
    own.wait()
    for copy in small:
        copy.wait()
    for stage, fresh in enumerate(stages):
        lax.fori_loop(bounds[stage], bounds[stage + 1], scatter, 0)
        if stage == last:
            take(0, range(last - 1))
            add(0)
        while arrived < needs[fresh[-1]]:
            sends[arrived - 1].wait_recv()
            arrived += 1
        correlate(stage, fresh)
    take(1, [last - 1])
    add(1)
    take(2, [last])

    load.wait()
    moment[...] = jnp.zeros_like(moment)

    def late(step, carry):
        for u in range(8):
            b = step * 8 + u
            line[pl.ds(b, 1), :] += multiply(b, [entries - 1])
        here = pl.ds(pl.multiple_of(step * 8, 8), 8)
        values = line[here, :]
        for c in range(cols):
            dens[c, here, :] = values[:, c * share:(c + 1) * share]
        part = jnp.sum(angular[:, here, :] * values[None], axis=2, keepdims=True)
        packed = moment.shape[0]
        low, high = part[:packed], part[part.shape[0] - packed:]
        moment[...] += jnp.sum(jnp.where(atoms[None] < NATOM, low, high) * member[here, :][None], axis=1)
        return carry

    lax.fori_loop(0, batches // 8, late, 0)

    def exchange(axis, place, size, src_of, dst_of, sent, received):
        copies = []
        for k in range(1, size):
            peer = lax.rem(place + k, size)
            copy = pltpu.make_async_remote_copy(
                src_ref=src_of(peer), dst_ref=dst_of(k),
                send_sem=sent.at[k - 1], recv_sem=received.at[k - 1],
                device_id={axis: peer}, device_id_type=MESH)
            copy.start()
            copies.append(copy)
        return copies

    moved = exchange("col", mine, cols, lambda peer: moment, lambda k: near.at[mine],
                     nsend_sem, nrecv_sem)
    near[mine] = moment[...]
    for copy in sends:
        copy.wait_send()
    for stage in range(len(stages)):
        for k in range(1, cols):
            norm_copy(stage, k).wait_send()
    for owner in range(cols):
        @pl.when(mine != owner)
        def _():
            for block in spots:
                if spots[block][0] == owner:
                    block_copy(block).wait_send()
    for copy in moved:
        copy.wait()
    total = near[0]
    for c in range(1, cols):
        total = total + near[c]
    moment[...] = total
    far[me] = total
    moved = exchange("row", me, rows, lambda peer: moment, lambda k: far.at[me],
                     fsend_sem, frecv_sem)
    copies = exchange("col", mine, cols, lambda peer: dens.at[peer], lambda k: got.at[k - 1],
                      dsend_sem, drecv_sem)
    result = dens[mine]
    for k, copy in enumerate(copies):
        copy.wait()
        result = result + got[k]
    out[...] = result
    for copy in moved:
        copy.wait()
    total = far[0]
    for r in range(1, rows):
        total = total + far[r]
    out_moments[...] = total


def finish(density, moments, out, out_moments):
    out[...] = density[...]
    packed, lm = moments.shape[0], out_moments.shape[0]
    out_moments[lm - packed:, :] = moments[:, NATOM:]
    out_moments[:packed, :] = moments[:, :NATOM]


def fused(coeffs, occupation, basis_on_grid, basis_map, basis_count, batch_atom, harmonics):
    batches, points, slots = basis_on_grid.shape
    owned, states = coeffs.shape
    rows, cols = lax.axis_size("row"), lax.axis_size("col")
    reach = rows * WIN
    groups = reach // LANES
    entries = len(KEPT[0])
    blocks = groups * (groups + 1) // 2
    stages = groups - 2
    vmem, dma = pltpu.VMEM, pltpu.SemaphoreType.DMA
    half, single, word = jnp.bfloat16, jnp.float32, jnp.int32
    whole = pl.BlockSpec(memory_space=pltpu.VMEM)
    lm = harmonics.shape[1]
    packed = (lm + 1) // 2
    apart = pl.BlockSpec(memory_space=pl.ANY)
    density, moments = pl.pallas_call(
        functools.partial(kernel, rows, cols, owned),
        out_shape=(jax.ShapeDtypeStruct((batches, points // cols), single),
                   jax.ShapeDtypeStruct((packed, LANES), single)),
        in_specs=[apart] * 7,
        out_specs=(whole, whole),
        scratch_shapes=[
            vmem((1, states), single),
            vmem((batches, slots), word),
            pltpu.SMEM((batches,), word),
            pltpu.SMEM((batches,), word),
            vmem((DEPTH, points, slots), half),
            vmem((len(USED[0]) * LANES, LANES), word),
            vmem((reach, states), half),
            vmem((groups, 2 * LANES, states), half),
            vmem((blocks, LANES, LANES), single),
            vmem((groups, LANES, LANES), single),
            vmem((groups, 8, LANES), single),
            vmem((stages, 8, LANES), single),
            vmem((blocks, LANES // 2, LANES), word),
            vmem((cols, 2 * entries, LANES // 2, LANES), word),
            vmem((cols, stages, 8, LANES), single),
            vmem((entries, 2 * LANES, 2 * LANES), half),
            vmem((batches, len(USED[0]) * LANES, points), half),
            vmem((lm, batches, points), single),
            vmem((batches, LANES), single),
            vmem((batches, points), single),
            vmem((cols, batches, points // cols), single),
            vmem((cols - 1, batches, points // cols), single),
            vmem((cols, packed, LANES), single),
            vmem((rows, packed, LANES), single),
            vmem((packed, LANES), single),
            dma((4,)), dma, dma((DEPTH,)), dma, dma((rows - 1,)), dma((rows - 1,)),
            dma((blocks,)), dma((cols, 2 * entries)), dma((stages, cols - 1)), dma((cols, stages)),
            dma((cols - 1,)), dma((cols - 1,)), dma((cols - 1,)), dma((cols - 1,)),
            dma((rows - 1,)), dma((rows - 1,)),
        ],
        compiler_params=pltpu.CompilerParams(
            collective_id=0, has_side_effects=True, vmem_limit_bytes=VMEM_BYTES),
    )(coeffs, occupation.reshape(1, -1), basis_on_grid, basis_map, basis_count,
      batch_atom, jnp.transpose(harmonics, (1, 0, 2)))
    density, moments = pl.pallas_call(
        finish, out_shape=(jax.ShapeDtypeStruct(density.shape, single),
                           jax.ShapeDtypeStruct((lm, NATOM), single)),
        in_specs=[whole, whole], out_specs=(whole, whole))(density, moments)
    return density, moments.T


def shards(coeffs, occupation, basis_on_grid, basis_map, basis_count, batch_atom, harmonics):
    batches, points, slots = basis_on_grid.shape
    owned, states = coeffs.shape
    rows, cols = lax.axis_size("row"), lax.axis_size("col")
    reach = rows * WIN
    share = points // cols
    needed = batches * reach * points * 2 + 10 * reach * states
    fits = needed < VMEM_BYTES * 3 // 4 and share % LANES == 0 and owned % WIN == 0
    if fits and rows == len(ORDER) and cols == len(KEPT) and reach == 6 * LANES and 2 * NATOM == LANES and batches % (2 * STEP) == 0:
        return fused(coeffs, occupation, basis_on_grid, basis_map, basis_count,
                     batch_atom, harmonics)
    density = plain(coeffs, occupation, basis_on_grid, basis_map, basis_count)
    part = lax.dynamic_slice_in_dim(harmonics, lax.axis_index("col") * share, share, 2)
    local_moment = jnp.sum(part * density[:, None, :], axis=2)
    atom_ids = lax.broadcasted_iota(jnp.int32, (batches, NATOM), 1)
    member = (batch_atom[:, None] == atom_ids).astype(jnp.float32)
    atom_part = jnp.dot(member.T, local_moment, precision=lax.Precision.HIGHEST)
    moments = lax.psum(atom_part, ("row", "col"))
    return (density, moments)


def solution(mesh):
    placed = (
        P("row", "col"),
        P("col"),
        P("row", None, None),
        P("row", None),
        P("row"),
        P("row"),
        P("row", None, None),
    )
    return jax.shard_map(
        shards, mesh=mesh, in_specs=placed, out_specs=(P("row", "col"), P()), check_vma=False
    )
```

```python
import functools

import jax
import jax.numpy as jnp
from jax import lax
from jax.experimental import pallas as pl
from jax.experimental.pallas import tpu as pltpu
from jax.sharding import PartitionSpec as P

WIN = 96
NATOM = 64
LANES = 128
VMEM_BYTES = 62 * 1024 * 1024
STEP = 4
DEPTH = 2 * STEP
STEPS = 32767.0
MARGIN = 1.0 + 2.0 ** -7
MESH = pl.DeviceIdType.MESH
ORDER = (0, 1, 2, 4, 3, 5, 6, 7)
KEPT = (
    ((0, (2, 3)), (1, (2, 3)), (1, (1,))),
    ((0, (0, 1)), (4, (0, 1)), (5, (0, 1))),
    ((2, (2, 3)), (4, (2, 3)), (5, (2, 3))),
    ((3, (3,)), (4, (4,)), (5, (4, 5))),
)
USED = ((0, 1, 2, 3), (0, 1, 4, 5), (2, 3, 4, 5), (2, 3, 4, 5))


def plain(coeffs, occupation, basis_on_grid, basis_map, basis_count):
    batches, points, slots = basis_on_grid.shape
    owned = coeffs.shape[0]
    owners = lax.axis_size("row")
    target = lax.broadcasted_iota(jnp.int32, (owners, WIN), 0)
    offset = lax.broadcasted_iota(jnp.int32, (owners, WIN), 1)
    outgoing_ids = jnp.mod(target * WIN + offset, owned).reshape(-1)
    outgoing = jnp.take(coeffs, outgoing_ids, axis=0)
    window = lax.all_to_all(outgoing, "row", split_axis=0, concat_axis=0, tiled=True)
    start = jnp.mod(lax.axis_index("row") * WIN, owned)
    source = basis_map // owned
    within = jnp.mod(basis_map % owned - start, owned)
    local_ids = source * WIN + within
    selected = jnp.take(window, local_ids, axis=0)
    slot_ids = lax.broadcasted_iota(jnp.int32, (batches, slots), 1)
    keep = slot_ids < basis_count[:, None]
    masked = jnp.where(keep[:, None, :], basis_on_grid, jnp.zeros_like(basis_on_grid))
    orbital = jnp.einsum("bps,bsk->bpk", masked, selected, preferred_element_type=jnp.float32)
    partial_density = jnp.sum(orbital * orbital * occupation[None, None, :], axis=2)
    full_density = lax.psum(partial_density, "col")
    share = points // lax.axis_size("col")
    return lax.dynamic_slice_in_dim(full_density, lax.axis_index("col") * share, share, 1)


def kernel(rows, cols, owned, coeffs, occ_in, basis, index_in, count_in, atom_in, harmonics, out, out_moments,
           occ, index, count, atom, held, names, window, split, local, scale_col, scale_row, norm, code, taken, norms, matrix,
           spread, angular, member, line, dens, got, near, far, moment,
           small_sem, own_sem, in_sem, angular_sem, send_sem, recv_sem, zsend_sem, zrecv_sem, vsend_sem, vrecv_sem,
           dsend_sem, drecv_sem, nsend_sem, nrecv_sem, fsend_sem, frecv_sem):
    batches, points, slots = basis.shape
    states = coeffs.shape[1]
    reach = rows * WIN
    groups = reach // LANES
    me, mine = lax.axis_index("row"), lax.axis_index("col")
    share = points // cols
    kept, entries = KEPT, len(KEPT[0])

    barrier = pltpu.get_barrier_semaphore()
    for k in range(1, rows):
        pl.semaphore_signal(barrier, inc=1, device_id={"row": lax.rem(me + k, rows)},
                            device_id_type=MESH)
    for k in range(1, cols):
        pl.semaphore_signal(barrier, inc=1, device_id={"col": lax.rem(mine + k, cols)},
                            device_id_type=MESH)

    def fetch(b, slot):
        return pltpu.make_async_copy(basis.at[b], held.at[slot], in_sem.at[slot])

    small = [pltpu.make_async_copy(src, dst, small_sem.at[n]) for n, (src, dst) in enumerate(
        ((count_in, count), (index_in, index), (atom_in, atom), (occ_in, occ)))]
    for copy in small:
        copy.start()
    for b in range(STEP):
        fetch(b, b).start()

    def chosen(values):
        total = values[0]
        for c in range(1, cols):
            total = jnp.where(mine == c, values[c], total)
        return total

    def rows_for(owner):
        return coeffs.at[pl.ds(pl.multiple_of(lax.rem(owner * WIN, owned), 32), WIN), :]

    def partner(k):
        bits = (lax.rem(me, 2), lax.rem(lax.div(me, 2), 2), lax.div(me, 4))
        return sum((1 - bit if k >> n & 1 else bit) * (1 << n) for n, bit in enumerate(bits))

    own = pltpu.make_async_copy(rows_for(me), window.at[0:WIN, :], own_sem)
    own.start()
    pl.semaphore_wait(barrier, rows + cols - 2)
    sends = []
    for p in range(1, rows):
        peer = partner(ORDER[p])
        copy = pltpu.make_async_remote_copy(
            src_ref=rows_for(peer), dst_ref=window.at[p * WIN:(p + 1) * WIN, :],
            send_sem=send_sem.at[p - 1], recv_sem=recv_sem.at[p - 1],
            device_id={"row": peer}, device_id_type=MESH)
        copy.start()
        sends.append(copy)
    load = pltpu.make_async_copy(harmonics, angular, angular_sem)
    load.start()

    start = lax.rem(me * WIN, owned)
    for r in range(len(USED[0])):
        row = lax.broadcasted_iota(jnp.int32, (LANES, LANES), 0) + chosen([g[r] for g in USED]) * LANES
        found = jnp.zeros_like(row)
        for p, k in enumerate(ORDER):
            own_row = row - p * WIN
            found = jnp.where((own_row >= 0) & (own_row < WIN), own_row + (start + partner(k) * owned), found)
        names[r * LANES:(r + 1) * LANES, :] = found
    lane = lax.broadcasted_iota(jnp.int32, (1, slots), 1)
    atoms = lax.broadcasted_iota(jnp.int32, (1, LANES), 1)
    matrix[...] = jnp.zeros_like(matrix)

    def scatter(step, carry):
        first = step * STEP
        base = lax.rem(step, 2) * STEP

        @pl.when(first + STEP < batches)
        def _():
            for u in range(STEP):
                fetch(first + STEP + u, STEP - base + u).start()

        for u in range(STEP):
            fetch(first + u, base + u).wait()
        for u in range(STEP):
            b = first + u
            ids = jnp.where(lane < count[b], index[pl.ds(b, 1), :], -1)
            hot = jnp.concatenate(
                [jnp.where(names[...] == ids[:, n:n + LANES], 1.0, 0.0) for n in range(0, slots, LANES)],
                axis=1).astype(jnp.bfloat16)
            moved = lax.dot_general(hot, held[base + u], (((1,), (1,)), ((), ())),
                                    preferred_element_type=jnp.float32)
            spread[b] = moved.astype(jnp.bfloat16)
            member[pl.ds(b, 1), :] = jnp.where(lax.rem(atoms, NATOM) == atom[b], 1.0, 0.0)
        return carry

    def group_rows(g):
        return slice(g * LANES, (g + 1) * LANES)

    spots = {}
    for owner in range(cols):
        for e, (i, js) in enumerate(kept[owner]):
            for h, j in enumerate(js):
                spots[i, j] = (owner, 2 * e + h)
    ids_of = {block: n for n, block in enumerate(spots)}

    def block_copy(block):
        owner, slot = spots[block]
        n = ids_of[block]
        return pltpu.make_async_remote_copy(
            src_ref=code.at[n], dst_ref=taken.at[mine, slot],
            send_sem=zsend_sem.at[n], recv_sem=zrecv_sem.at[mine, slot],
            device_id={"col": owner}, device_id_type=MESH)

    def norm_copy(stage, k):
        return pltpu.make_async_remote_copy(
            src_ref=norm.at[stage], dst_ref=norms.at[mine, stage],
            send_sem=vsend_sem.at[stage, k - 1], recv_sem=vrecv_sem.at[mine, stage],
            device_id={"col": lax.rem(mine + k, cols)}, device_id_type=MESH)

    def correlate(stage, fresh):
        tile_row = lax.broadcasted_iota(jnp.int32, (8, LANES), 0)
        tile = jnp.zeros((8, LANES), jnp.float32)
        for g in fresh:
            wide = window[group_rows(g), :].astype(jnp.float32)
            scaled = wide * occ[...]
            high = scaled.astype(jnp.bfloat16)
            split[g, 0:LANES, :] = high
            split[g, LANES:2 * LANES, :] = (scaled - high.astype(jnp.float32)).astype(jnp.bfloat16)
            square = jnp.sum(scaled * wide, axis=1, keepdims=True)
            root = jnp.where(square > 0.0, lax.rsqrt(square), 0.0)
            inverse = jnp.broadcast_to(root * (1.0 / MARGIN), (LANES, LANES))
            scale_col[g] = inverse
            scale_row[g] = inverse.T[0:8, :]
            length = jnp.broadcast_to(square * root * MARGIN, (LANES, LANES)).T
            tile = jnp.where(tile_row == g, length[0:8, :], tile)
        norm[stage] = tile
        for k in range(1, cols):
            norm_copy(stage, k).start()
        made = {}
        for j in fresh:
            for first in range(0, j + 1, 2):
                lanes = range(first, min(first + 2, j + 1))
                right = window[first * LANES:(lanes[-1] + 1) * LANES, :]
                both = lax.dot_general(split[j], right, (((1,), (1,)), ((), ())),
                                       preferred_element_type=jnp.float32)
                value = both[0:LANES, :] + both[LANES:2 * LANES, :]
                for n, i in enumerate(lanes):
                    made[i, j] = value[:, group_rows(n)]
        ready = [block for block in spots if max(block) in fresh]
        for i, j in ready:
            value = made[i, j] if i <= j else made[j, i].T
            n = ids_of[i, j]
            local[n] = value
            ratio = value * scale_col[j] * scale_row[i, 0:1, :]
            steps = jnp.round(ratio * STEPS).astype(jnp.int32)
            half = LANES // 2
            code[n] = (steps[0:half, :] << 16) | (steps[half:, :] & 0xFFFF)
        for owner in range(cols):
            @pl.when(mine != owner)
            def _():
                for block in ready:
                    if spots[block][0] == owner:
                        block_copy(block).start()

    def collect(owner, es):
        others = [s for s in range(cols) if s != owner]
        for e in es:
            i, js = kept[owner][e]
            for h, j in enumerate(js):
                slot = 2 * e + h
                value = local[ids_of[i, j]]
                for s in others:
                    pltpu.make_async_remote_copy(
                        src_ref=code.at[0], dst_ref=taken.at[s, slot],
                        send_sem=zsend_sem.at[0], recv_sem=zrecv_sem.at[s, slot],
                        device_id={"col": s}, device_id_type=MESH).wait_recv()
                    word = taken[s, slot]
                    steps = jnp.concatenate([word >> 16, (word << 16) >> 16], axis=0)
                    down = norms[s, stage_of(j), j:j + 1, :] * (1.0 / STEPS)
                    down = jnp.broadcast_to(down, (LANES, LANES)).T
                    value = value + steps.astype(jnp.float32) * down * norms[s, stage_of(i), i:i + 1, :]
                if i != j:
                    value = value + value
                high = value.astype(jnp.bfloat16)
                low = (value - high.astype(jnp.float32)).astype(jnp.bfloat16)
                matrix[e, group_rows(h), 0:LANES] = high
                matrix[e, group_rows(h), LANES:2 * LANES] = low

    needs = [-(-(g + 1) * LANES // WIN) for g in range(groups)]
    stages = [[0, 1, 2]] + [[g] for g in range(3, groups)]

    def stage_of(g):
        return next(n for n, fresh in enumerate(stages) if g in fresh)

    def await_norms(owner, which):
        for stage in which:
            for s in range(cols):
                if s != owner:
                    pltpu.make_async_remote_copy(
                        src_ref=norm.at[stage], dst_ref=norms.at[s, stage],
                        send_sem=vsend_sem.at[stage, 0], recv_sem=vrecv_sem.at[s, stage],
                        device_id={"col": s}, device_id_type=MESH).wait_recv()

    def group_of(b, g):
        return spread[b, pl.ds(pl.multiple_of(g * LANES, LANES), LANES), :]

    def multiply(b, es):
        total = jnp.zeros((8, points), jnp.float32)
        for e in es:
            i = chosen([USED[c].index(kept[c][e][0]) for c in range(cols)])
            right = group_of(b, i)
            product = lax.dot_general(matrix[e], jnp.concatenate([right, right], axis=0),
                                      (((1,), (0,)), ((), ())), preferred_element_type=jnp.float32)
            for h in range(2):
                j = chosen([USED[c].index(kept[c][e][1][min(h, len(kept[c][e][1]) - 1)]) for c in range(cols)])
                term = product[group_rows(h), :] * group_of(b, j).astype(jnp.float32)
                total = total + jnp.sum(term.reshape(LANES // 8, 8, points), axis=0)
        return jnp.sum(total, axis=0, keepdims=True)

    def take(e, which):
        for owner in range(cols):
            @pl.when(mine == owner)
            def _():
                await_norms(owner, which)
                collect(owner, [e])

    def add(e):
        def body(step, carry):
            for u in range(8):
                b = step * 8 + u
                value = multiply(b, [e])
                line[pl.ds(b, 1), :] = value if e == 0 else line[pl.ds(b, 1), :] + value
            return carry

        lax.fori_loop(0, batches // 8, body, 0)

    last = len(stages) - 1
    bounds = [batches // STEP * n // 10 for n in (0, 3, 6, 10, 10)]
    arrived = 1
    own.wait()
    for copy in small:
        copy.wait()
    for stage, fresh in enumerate(stages):
        lax.fori_loop(bounds[stage], bounds[stage + 1], scatter, 0)
        if stage == last:
            take(0, range(last - 1))
            add(0)
        while arrived < needs[fresh[-1]]:
            sends[arrived - 1].wait_recv()
            arrived += 1
        correlate(stage, fresh)
    take(1, [last - 1])
    add(1)
    take(2, [last])

    load.wait()
    moment[...] = jnp.zeros_like(moment)

    def late(step, carry):
        for u in range(8):
            b = step * 8 + u
            line[pl.ds(b, 1), :] += multiply(b, [entries - 1])
        here = pl.ds(pl.multiple_of(step * 8, 8), 8)
        values = line[here, :]
        for c in range(cols):
            dens[c, here, :] = values[:, c * share:(c + 1) * share]
        part = jnp.sum(angular[:, here, :] * values[None], axis=2, keepdims=True)
        packed = moment.shape[0]
        low, high = part[:packed], part[part.shape[0] - packed:]
        moment[...] += jnp.sum(jnp.where(atoms[None] < NATOM, low, high) * member[here, :][None], axis=1)
        return carry

    lax.fori_loop(0, batches // 8, late, 0)

    def exchange(axis, place, size, src_of, dst_of, sent, received):
        copies = []
        for k in range(1, size):
            peer = lax.rem(place + k, size)
            copy = pltpu.make_async_remote_copy(
                src_ref=src_of(peer), dst_ref=dst_of(k),
                send_sem=sent.at[k - 1], recv_sem=received.at[k - 1],
                device_id={axis: peer}, device_id_type=MESH)
            copy.start()
            copies.append(copy)
        return copies

    moved = exchange("col", mine, cols, lambda peer: moment, lambda k: near.at[mine],
                     nsend_sem, nrecv_sem)
    near[mine] = moment[...]
    for copy in sends:
        copy.wait_send()
    for stage in range(len(stages)):
        for k in range(1, cols):
            norm_copy(stage, k).wait_send()
    for owner in range(cols):
        @pl.when(mine != owner)
        def _():
            for block in spots:
                if spots[block][0] == owner:
                    block_copy(block).wait_send()
    for copy in moved:
        copy.wait()
    total = near[0]
    for c in range(1, cols):
        total = total + near[c]
    moment[...] = total
    far[me] = total
    moved = exchange("row", me, rows, lambda peer: moment, lambda k: far.at[me],
                     fsend_sem, frecv_sem)
    copies = exchange("col", mine, cols, lambda peer: dens.at[peer], lambda k: got.at[k - 1],
                      dsend_sem, drecv_sem)
    result = dens[mine]
    for k, copy in enumerate(copies):
        copy.wait()
        result = result + got[k]
    out[...] = result
    for copy in moved:
        copy.wait()
    total = far[0]
    for r in range(1, rows):
        total = total + far[r]
    out_moments[...] = total


def finish(density, moments, out, out_moments):
    out[...] = density[...]
    packed, lm = moments.shape[0], out_moments.shape[0]
    out_moments[lm - packed:, :] = moments[:, NATOM:]
    out_moments[:packed, :] = moments[:, :NATOM]


def fused(coeffs, occupation, basis_on_grid, basis_map, basis_count, batch_atom, harmonics):
    batches, points, slots = basis_on_grid.shape
    owned, states = coeffs.shape
    rows, cols = lax.axis_size("row"), lax.axis_size("col")
    reach = rows * WIN
    groups = reach // LANES
    entries = len(KEPT[0])
    blocks = groups * (groups + 1) // 2
    stages = groups - 2
    vmem, dma = pltpu.VMEM, pltpu.SemaphoreType.DMA
    half, single, word = jnp.bfloat16, jnp.float32, jnp.int32
    whole = pl.BlockSpec(memory_space=pltpu.VMEM)
    lm = harmonics.shape[1]
    packed = (lm + 1) // 2
    apart = pl.BlockSpec(memory_space=pl.ANY)
    density, moments = pl.pallas_call(
        functools.partial(kernel, rows, cols, owned),
        out_shape=(jax.ShapeDtypeStruct((batches, points // cols), single),
                   jax.ShapeDtypeStruct((packed, LANES), single)),
        in_specs=[apart] * 7,
        out_specs=(whole, whole),
        scratch_shapes=[
            vmem((1, states), single),
            vmem((batches, slots), word),
            pltpu.SMEM((batches,), word),
            pltpu.SMEM((batches,), word),
            vmem((DEPTH, points, slots), half),
            vmem((len(USED[0]) * LANES, LANES), word),
            vmem((reach, states), half),
            vmem((groups, 2 * LANES, states), half),
            vmem((blocks, LANES, LANES), single),
            vmem((groups, LANES, LANES), single),
            vmem((groups, 8, LANES), single),
            vmem((stages, 8, LANES), single),
            vmem((blocks, LANES // 2, LANES), word),
            vmem((cols, 2 * entries, LANES // 2, LANES), word),
            vmem((cols, stages, 8, LANES), single),
            vmem((entries, 2 * LANES, 2 * LANES), half),
            vmem((batches, len(USED[0]) * LANES, points), half),
            vmem((lm, batches, points), single),
            vmem((batches, LANES), single),
            vmem((batches, points), single),
            vmem((cols, batches, points // cols), single),
            vmem((cols - 1, batches, points // cols), single),
            vmem((cols, packed, LANES), single),
            vmem((rows, packed, LANES), single),
            vmem((packed, LANES), single),
            dma((4,)), dma, dma((DEPTH,)), dma, dma((rows - 1,)), dma((rows - 1,)),
            dma((blocks,)), dma((cols, 2 * entries)), dma((stages, cols - 1)), dma((cols, stages)),
            dma((cols - 1,)), dma((cols - 1,)), dma((cols - 1,)), dma((cols - 1,)),
            dma((rows - 1,)), dma((rows - 1,)),
        ],
        compiler_params=pltpu.CompilerParams(
            collective_id=0, has_side_effects=True, vmem_limit_bytes=VMEM_BYTES),
    )(coeffs, occupation.reshape(1, -1), basis_on_grid, basis_map, basis_count,
      batch_atom, jnp.transpose(harmonics, (1, 0, 2)))
    density, moments = pl.pallas_call(
        finish, out_shape=(jax.ShapeDtypeStruct(density.shape, single),
                           jax.ShapeDtypeStruct((lm, NATOM), single)),
        in_specs=[whole, whole], out_specs=(whole, whole))(density, moments)
    return density, moments.T


def shards(coeffs, occupation, basis_on_grid, basis_map, basis_count, batch_atom, harmonics):
    batches, points, slots = basis_on_grid.shape
    owned, states = coeffs.shape
    rows, cols = lax.axis_size("row"), lax.axis_size("col")
    reach = rows * WIN
    share = points // cols
    needed = batches * reach * points * 2 + 10 * reach * states
    fits = needed < VMEM_BYTES * 3 // 4 and share % LANES == 0 and owned % WIN == 0
    if fits and rows == len(ORDER) and cols == len(KEPT) and reach == 6 * LANES and 2 * NATOM == LANES and batches % (2 * STEP) == 0:
        return fused(coeffs, occupation, basis_on_grid, basis_map, basis_count,
                     batch_atom, harmonics)
    density = plain(coeffs, occupation, basis_on_grid, basis_map, basis_count)
    part = lax.dynamic_slice_in_dim(harmonics, lax.axis_index("col") * share, share, 2)
    local_moment = jnp.sum(part * density[:, None, :], axis=2)
    atom_ids = lax.broadcasted_iota(jnp.int32, (batches, NATOM), 1)
    member = (batch_atom[:, None] == atom_ids).astype(jnp.float32)
    atom_part = jnp.dot(member.T, local_moment, precision=lax.Precision.HIGHEST)
    moments = lax.psum(atom_part, ("row", "col"))
    return (density, moments)


def solution(mesh):
    placed = (
        P("row", "col"),
        P("col"),
        P("row", None, None),
        P("row", None),
        P("row"),
        P("row"),
        P("row", None, None),
    )
    return jax.shard_map(
        shards, mesh=mesh, in_specs=placed, out_specs=(P("row", "col"), P()), check_vma=False
    )
```
